1024 devices in a mesh: mem: 16 (over x_hi, y), band: 64 (over x_lo, z, core).
Axes of the slice: x: 8 (x_hi: 2, x_lo: 4; x = x_hi * 4 + x_lo), y: 8, z: 8, core: 2. Of those that a mesh axis runs over, the one named last changes fastest.
Arguments:
- prior_collection: float32 [512, 3, 512, 256], P('mem', None, 'band'), may hold values from -3 to 3
- obs_index: int32 [64, 16, 256], P('band'), may hold values from 0 to 1151
- obs_values: float32 [64, 16, 256], P('band', 'mem'), may hold values from -6 to 6
- obs_var: float32 [64, 16, 256], P('band', 'mem'), may hold values from 0.1 to 1
Outputs:
- analysis: float32 [512, 3, 512, 256], P('mem', None, 'band')
The draws below stay inside these ranges and needn't reach their ends.
Inputs may be any that keep to these rules, and one draw needn't show every extreme that they name: obs_index[b, p, i] is field * 3 * 8 * 16 + row * 3 * 16 + c, a position in the window of patch p of band b.
All inputs are finite; a program needn't handle non-finite values. Where the reference program divides by a largest or mean magnitude, that divisor is 1e-20 or more.
Results may differ from the reference program's by a relative error of at most 0.0022.
Values may be sent and summed in bfloat16 or wider, within the bound.
No kernel may reach another device: no remote copies, remote signals or barrier semaphores. Data moves between devices by JAX's collectives and lax.ppermute only.
A program may use at most 64 MiB of HBM per device.

```python
import math
import jax
import jax.numpy as jnp
from jax import lax

MEMBERS = 512
PARALLELS_IN_ZONE = 8
COLS = 256
NOBS = 256
STEPS = 3
NEWTON = 3
BANDS = 64
PATCHES = 16
PCOL = 16
NROWS = 512


def place_ends(values, rng, smallest, high):
    longest = values.shape.index(max(values.shape))
    spots = []
    for shift in (0, 1):
        where = [jax.random.randint(jax.random.fold_in(rng, axis), (), 0, length) for axis, length in enumerate(values.shape)]
        where[longest] = (where[longest] + shift) % values.shape[longest]
        spots.append(tuple(where))
    return values.at[spots[0]].set(smallest).at[spots[1]].set(high)


def levels(rng, shape, pieces, least, top_value):
    level = 1.0
    for position, shards_of in pieces:
        steps = jax.random.uniform(jax.random.fold_in(jax.random.fold_in(rng, 6), position), (shards_of,), jnp.float32, least / len(pieces), top_value / len(pieces))
        level = level * jnp.repeat(jnp.exp(steps), shape[position] // shards_of).reshape((-1,) + (1,) * (len(shape) - 1 - position))
    return level


def noise(stream_key, dims, scale, limit, shards=(), kind=jnp.bfloat16):
    factor_of = levels(stream_key, dims, shards, -0.22, 0.18) if shards else 1.0
    entries = jax.random.normal(stream_key, dims, jnp.float32) * scale * factor_of
    return jnp.minimum(jnp.maximum(entries, -limit), limit).astype(kind)


def setup_inputs(seed: int = 0) -> dict:
    key_list = jax.random.split(jax.random.key(seed), 5)
    prior_collection = noise(key_list[0], (MEMBERS, 3, NROWS, COLS), 0.5, 3.0, ((0, 16), (2, 64)), jnp.float32)
    obs_index = place_ends(jax.random.randint(key_list[1], (BANDS, PATCHES, NOBS), 0, 9 * PARALLELS_IN_ZONE * PCOL), jax.random.fold_in(key_list[1], 1), 0, (9 * PARALLELS_IN_ZONE * PCOL) - 1).astype(jnp.int32)
    obs_values = noise(key_list[2], (BANDS, PATCHES, NOBS), 1.0, 6.0, ((0, 64), (1, 16)), jnp.float32)
    obs_var = jnp.clip(jnp.exp(math.log(1.0) - 2.3025851 * jax.random.uniform(key_list[3], (BANDS, PATCHES, NOBS), jnp.float32) ** levels(key_list[3], (BANDS, PATCHES, NOBS), ((0, 64), (1, 16)), -0.2, 0.2)), 0.1, 1.0)
    return {"prior_collection": prior_collection, "obs_index": obs_index, "obs_values": obs_values, "obs_var": obs_var}


time_step = 0.1
gravity = 1.0
coriolis = 0.05
mean_depth = 1.0

def east_west(field):
    return (jnp.roll(field, -1, -1) - jnp.roll(field, 1, -1)) * 0.5

def north_south(field):
    padded = jnp.pad(field, ((1, 1), (0, 0)))
    return (padded[2:] - padded[:-2]) * 0.5

def advance(fluid_layer_fields):
    height, eastward, northward = (fluid_layer_fields[0], fluid_layer_fields[1], fluid_layer_fields[2])
    new_height = height - time_step * (east_west((mean_depth + height) * eastward) + north_south((mean_depth + height) * northward))
    new_east = eastward - time_step * (gravity * east_west(new_height) + eastward * east_west(eastward) + northward * north_south(eastward)) + coriolis * northward
    new_north = northward - time_step * (gravity * north_south(new_height) + eastward * east_west(northward) + northward * north_south(northward)) - coriolis * eastward
    return jnp.stack([new_height, new_east, new_north])

def single_prediction(fluid_layer_fields):
    for repeat in range(STEPS):
        fluid_layer_fields = advance(fluid_layer_fields)
    return fluid_layer_fields

def analyse(patch_state, observed, indices, values, variances, window_width):
    members = patch_state.shape[0]
    highest = lax.Precision.HIGHEST
    observed_wide = observed.astype(jnp.float32)
    obs_mean = lax.optimization_barrier(jnp.mean(observed_wide, axis=0))
    perturb = (observed_wide - obs_mean).astype(jnp.bfloat16)
    window_column = (indices % window_width).astype(jnp.float32)
    patch_width = window_width // 3
    taper_weight = jnp.exp(-0.5 * ((window_column - (window_width - 1) * 0.5) / patch_width) ** 2)
    obs_weight = taper_weight / variances
    weighted = (perturb.astype(jnp.float32) * obs_weight).astype(jnp.bfloat16)
    gram_matrix = lax.dot_general(weighted, perturb, (((1,), (1,)), ((), ())), preferred_element_type=jnp.float32)
    unit_matrix = jnp.eye(members, dtype=jnp.float32)
    system = (members - 1) * unit_matrix + gram_matrix
    norm_bound = jnp.max(lax.optimization_barrier(jnp.sum(jnp.abs(system), axis=1)))
    iterate = system / norm_bound
    inverse = unit_matrix
    for newton_turn in range(NEWTON):
        if newton_turn == 0:
            middle = 1.5 * unit_matrix - 0.5 * iterate
            inverse = middle
        else:
            middle = 1.5 * unit_matrix - 0.5 * jnp.dot(inverse, iterate, precision=highest)
            inverse = jnp.dot(middle, inverse, precision=highest)
        if newton_turn + 1 < NEWTON:
            iterate = jnp.dot(iterate, middle, precision=highest)
    inverse_root = inverse / jnp.sqrt(norm_bound)
    innovation = obs_weight * (values - obs_mean)
    pulled = jnp.dot(perturb.astype(jnp.float32), innovation, precision=highest)
    mean_weight = jnp.dot(inverse_root, jnp.dot(inverse_root, pulled, precision=highest), precision=highest)
    weights = math.sqrt(members - 1) * inverse_root + mean_weight[:, None]
    state_mean = lax.optimization_barrier(jnp.mean(patch_state, axis=0))
    spread = patch_state - state_mean
    return state_mean + lax.dot_general(weights, spread, (((0,), (0,)), ((), ())), precision=highest, preferred_element_type=jnp.float32)

def reference(prior_collection, obs_index, obs_values, obs_var):
    predicted_fields_all = lax.map(single_prediction, prior_collection)
    quantised_entry = predicted_fields_all.astype(jnp.bfloat16)
    window_width = 3 * PCOL

    def one_patch(patch_number):
        band_number = patch_number // PATCHES
        patch_place = patch_number % PATCHES
        first_parallel_index = (band_number * PARALLELS_IN_ZONE).astype(jnp.int32)
        zonal_strip_parallels = lax.dynamic_slice_in_dim(predicted_fields_all, first_parallel_index, PARALLELS_IN_ZONE, 2)
        band_rounded = lax.dynamic_slice_in_dim(quantised_entry, first_parallel_index, PARALLELS_IN_ZONE, 2)
        columns = (patch_place * PCOL - PCOL + jnp.arange(window_width, dtype=jnp.int32)) % COLS
        window = jnp.take(band_rounded, columns.astype(jnp.int32), axis=3).reshape(MEMBERS, -1)
        indices = obs_index[band_number, patch_place]
        observed = jnp.take(window, indices, axis=1)
        own_cells = lax.dynamic_slice_in_dim(zonal_strip_parallels, (patch_place * PCOL).astype(jnp.int32), PCOL, 3).reshape(MEMBERS, -1)
        result = analyse(own_cells, observed, indices, obs_values[band_number, patch_place], obs_var[band_number, patch_place], window_width)
        return result.reshape(MEMBERS, 3, PARALLELS_IN_ZONE, PCOL)
    patches_out = lax.map(one_patch, jnp.arange(BANDS * PATCHES, dtype=jnp.int32))
    patches_out = patches_out.reshape(BANDS, PATCHES, MEMBERS, 3, PARALLELS_IN_ZONE, PCOL)
    return patches_out.transpose(2, 3, 0, 4, 1, 5).reshape(MEMBERS, 3, NROWS, COLS)
```

```python
import math

import jax
import jax.numpy as jnp
from jax import lax
from jax.experimental import pallas as pl
from jax.experimental.pallas import tpu as pltpu
from jax.sharding import PartitionSpec as P

STEPS = 3
NEWTON = 3
HALO = 2 * STEPS

time_step = 0.1
gravity = 1.0
coriolis = 0.05
mean_depth = 1.0

GROUP = 8
LANES = 128
BLOCK = 16


def tiled_view(x):
    m, f, r, c = x.shape
    halves = c // LANES
    return x.reshape(m, f, r, halves, LANES).transpose(0, 1, 3, 2, 4).reshape(-1, LANES)


def untiled_view(x, shape):
    m, f, r, c = shape
    halves = c // LANES
    return x.reshape(m, f, halves, r, LANES).transpose(0, 1, 3, 2, 4).reshape(shape)


def block_transpose(tiles):
    tiles = list(tiles)
    block = lax.broadcasted_iota(jnp.int32, tiles[0].shape, 1) // BLOCK
    for s in (4, 2, 1):
        high = (block & s) != 0
        for i in range(8):
            if i & s:
                continue
            a, b = tiles[i], tiles[i + s]
            tiles[i] = jnp.where(high, pltpu.roll(b, BLOCK * s, 1), a)
            tiles[i + s] = jnp.where(high, b, pltpu.roll(a, LANES - BLOCK * s, 1))
    return tiles


def edges_kernel(prior_ref, first_ref, last_ref):
    fields, rows = 3, 8
    stride = fields * rows * 2
    for member in range(0, first_ref.shape[1], 2 * GROUP):
        for f in range(fields):
            for half in range(2):
                lanes = slice(half * LANES, (half + 1) * LANES)
                for row in range(rows):
                    parts = [
                        prior_ref[pl.ds((m * fields + f) * 2 * rows + half * rows + row, GROUP, stride=stride), :]
                        for m in (member, member + GROUP)
                    ]
                    both = jnp.concatenate(parts, axis=0).astype(jnp.bfloat16)
                    if row < HALO:
                        first_ref[f * HALO + row, member : member + 2 * GROUP, lanes] = both
                    if row >= rows - HALO:
                        last_ref[f * HALO + row - (rows - HALO), member : member + 2 * GROUP, lanes] = both


def east_west(x):
    cols = x.shape[-1]
    return (pltpu.roll(x, cols - 1, 1) - pltpu.roll(x, 1, 1)) * 0.5


def forecast_kernel(inside_ref, prior_ref, above_ref, below_ref, index_ref, state_ref, observed_ref, ping, pong, window):
    fields, rows = 3, 8
    deep = rows + 2 * HALO
    stride = fields * rows * 2
    members = state_ref.shape[1]
    patches = state_ref.shape[0]
    above_in = inside_ref[0]
    below_in = inside_ref[1]

    for f in range(fields):
        for row in range(HALO):
            ping[f * deep + row] = above_ref[f * HALO + row].astype(jnp.float32)
            ping[f * deep + HALO + rows + row] = below_ref[f * HALO + row].astype(jnp.float32)

    for member in range(0, members, GROUP):
        here = slice(member, member + GROUP)
        for f in range(fields):
            for half in range(2):
                for row in range(rows):
                    start = (member * fields + f) * 2 * rows + half * rows + row
                    ping[f * deep + HALO + row, here, half * LANES : (half + 1) * LANES] = prior_ref[
                        pl.ds(start, GROUP, stride=stride), :
                    ]

    def one_group(g, carry):
        here = pl.ds(pl.multiple_of(g * GROUP, GROUP), GROUP)

        def masked(x, row):
            if row < HALO:
                return x * above_in
            if row >= HALO + rows:
                return x * below_in
            return x

        src, dst = ping, pong
        for turn in range(STEPS):
            low = 2 * (turn + 1)
            high = deep - 2 * (turn + 1)

            def get(f, row, src=src):
                return src[f * deep + row, here, :]

            north_flux = {}

            def flux(row, get=get, north_flux=north_flux):
                if row not in north_flux:
                    north_flux[row] = (mean_depth + get(0, row)) * get(2, row)
                return north_flux[row]

            def new_height(row, get=get, flux=flux):
                height = get(0, row)
                flux_east = (mean_depth + height) * get(1, row)
                value = height - time_step * (
                    east_west(flux_east) + (flux(row + 1) - flux(row - 1)) * 0.5
                )
                return masked(value, row)

            heights = {row: new_height(row) for row in (low - 1, low)}
            for row in range(low, high):
                heights[row + 1] = new_height(row + 1)
                east = get(1, row)
                north = get(2, row)
                east_slope = (get(1, row + 1) - get(1, row - 1)) * 0.5
                north_slope = (get(2, row + 1) - get(2, row - 1)) * 0.5
                height_slope = (heights[row + 1] - heights[row - 1]) * 0.5
                new_east = (
                    east
                    - time_step * (gravity * east_west(heights[row]) + east * east_west(east) + north * east_slope)
                    + coriolis * north
                )
                new_north = (
                    north
                    - time_step * (gravity * height_slope + east * east_west(north) + north * north_slope)
                    - coriolis * east
                )
                dst[row, here, :] = heights[row]
                dst[deep + row, here, :] = masked(new_east, row)
                dst[2 * deep + row, here, :] = masked(new_north, row)
                del heights[row - 1]
            src, dst = dst, src

        for f in range(fields):
            for half in range(2):
                lanes = slice(half * LANES, (half + 1) * LANES)
                tiles = [src[f * deep + HALO + row, here, lanes] for row in range(rows)]
                for p, tile in enumerate(block_transpose(tiles)):
                    state_ref[half * 8 + p, here, f * LANES : (f + 1) * LANES] = tile
        return carry

    lax.fori_loop(0, members // GROUP, one_group, 0)

    for p in range(patches):
        window[p] = state_ref[p].astype(jnp.bfloat16)
    cells = fields * LANES
    spot_of = lax.broadcasted_iota(jnp.int32, (cells, index_ref.shape[1]), 0)
    for p in range(patches):
        index = index_ref[p : p + 1, :]
        field_row = (index * 1366) >> 16
        column = index - field_row * (3 * BLOCK)
        part = column >> 4
        spot = field_row * BLOCK + (column & (BLOCK - 1))
        total = None
        for k in range(3):
            wanted = jnp.where(part == k, spot, -1)
            chosen = jnp.where(spot_of == wanted, 1.0, 0.0).astype(jnp.bfloat16)
            piece = jnp.dot(window[(p + k - 1) % patches], chosen, preferred_element_type=jnp.float32)
            total = piece if total is None else total + piece
        observed_ref[p] = total.astype(jnp.bfloat16)


def split(x):
    high = x.astype(jnp.bfloat16)
    return high, (x - high.astype(jnp.float32)).astype(jnp.bfloat16)


def mul3(a, b):
    def dot(x, y):
        return jnp.dot(x, y, preferred_element_type=jnp.float32)

    return dot(a[0], b[0]) + (dot(a[0], b[1]) + dot(a[1], b[0]))


def three_rows(x):
    high = x.astype(jnp.bfloat16).astype(jnp.float32)
    rest = x - high
    middle = rest.astype(jnp.bfloat16).astype(jnp.float32)
    low = rest - middle
    shape = (16, x.shape[1])
    row = lax.broadcasted_iota(jnp.int32, shape, 0)
    stacked = jnp.where(row == 0, high, jnp.where(row == 1, middle, jnp.where(row == 2, low, 0.0)))
    return stacked.astype(jnp.bfloat16)


def weights_kernel(observed_ref, index_ref, values_ref, var_ref, high_ref, low_ref):
    members = observed_ref.shape[0]
    wide = observed_ref[...].astype(jnp.float32)
    obs_mean = jnp.sum(wide, axis=0, keepdims=True) * (1.0 / members)
    perturb = (wide - obs_mean).astype(jnp.bfloat16)
    index = index_ref[...]
    column = (index - ((index * 1366) >> 16) * (3 * BLOCK)).astype(jnp.float32)
    taper = jnp.exp(-0.5 * jnp.square((column - (3 * BLOCK - 1) * 0.5) / BLOCK))
    obs_weight = taper / var_ref[...]
    weighted = (perturb.astype(jnp.float32) * obs_weight).astype(jnp.bfloat16)
    contract = (((1,), (1,)), ((), ()))
    gram = lax.dot_general(perturb, weighted, contract, preferred_element_type=jnp.float32)
    row = lax.broadcasted_iota(jnp.int32, (members, members), 0)
    col = lax.broadcasted_iota(jnp.int32, (members, members), 1)
    unit = jnp.where(row == col, 1.0, 0.0)
    system = (members - 1) * unit + gram
    norm_bound = jnp.max(jnp.sum(jnp.abs(system), axis=0, keepdims=True), axis=1, keepdims=True)
    iterate = system / norm_bound
    middle = 1.5 * unit - 0.5 * iterate
    inverse_parts = split(middle)
    iterate_parts = split(mul3(split(iterate), inverse_parts))
    inverse = None
    for turn in range(1, NEWTON):
        middle_parts = split(1.5 * unit - 0.5 * mul3(inverse_parts, iterate_parts))
        inverse = mul3(middle_parts, inverse_parts)
        inverse_parts = split(inverse)
        if turn + 1 < NEWTON:
            iterate_parts = split(mul3(iterate_parts, middle_parts))

    def through(x):
        rows = three_rows(x)
        both = jnp.dot(rows, inverse_parts[0], preferred_element_type=jnp.float32) + jnp.dot(
            rows, inverse_parts[1], preferred_element_type=jnp.float32
        )
        return jnp.sum(both, axis=0, keepdims=True)

    innovation = obs_weight * (values_ref[...] - obs_mean)
    pulled = jnp.sum(
        lax.dot_general(three_rows(innovation), perturb, contract, preferred_element_type=jnp.float32),
        axis=0,
        keepdims=True,
    )
    mean_weight = through(through(pulled)) / norm_bound
    weights = (math.sqrt(members - 1) * lax.rsqrt(norm_bound)) * inverse + mean_weight
    high_ref[...], low_ref[...] = split(weights)


def update_kernel(state_ref, high_ref, low_ref, out_ref):
    state = state_ref[...]
    state_mean = jnp.sum(state, axis=0, keepdims=True) * (1.0 / state.shape[0])
    spread = split(state - state_mean)
    out_ref[...] = state_mean + mul3((high_ref[...], low_ref[...]), spread)


def unpack_kernel(returned_ref, out_ref):
    fields, rows = 3, 8
    stride = fields * rows * 2
    for f in range(fields):
        for half in range(2):
            tiles = [returned_ref[half * 8 + p, :, f * LANES : (f + 1) * LANES] for p in range(8)]
            for r, tile in enumerate(block_transpose(tiles)):
                out_ref[pl.ds(f * 2 * rows + half * rows + r, GROUP, stride=stride), :] = tile


def body(prior_collection, obs_index, obs_values, obs_var):
    members_here, fields, rows, cols = prior_collection.shape
    bands = lax.axis_size("band")
    patches = lax.axis_size("mem")
    members = members_here * patches
    nobs = obs_index.shape[-1]
    cells = fields * rows * BLOCK
    f32, bf16 = jnp.float32, jnp.bfloat16
    shaped = jax.ShapeDtypeStruct
    prior = tiled_view(prior_collection)

    halo_shape = (fields * HALO, members_here, cols)
    first, last = pl.pallas_call(
        edges_kernel, out_shape=(shaped(halo_shape, bf16), shaped(halo_shape, bf16)), name="edges"
    )(prior)
    up = [(i, i + 1) for i in range(bands - 1)]
    down = [(j, i) for i, j in up]
    above = lax.ppermute(last, "band", up)
    below = lax.ppermute(first, "band", down)

    band = lax.axis_index("band")
    inside = jnp.stack([band > 0, band < bands - 1]).astype(f32)
    vmem = pl.BlockSpec(memory_space=pltpu.VMEM)
    smem = pl.BlockSpec(memory_space=pltpu.SMEM)
    deep = (fields * (rows + 2 * HALO), members_here, cols)
    state, observed = pl.pallas_call(
        forecast_kernel,
        in_specs=[smem, vmem, vmem, vmem, vmem],
        out_shape=(shaped((patches, members_here, cells), f32), shaped((patches, members_here, nobs), bf16)),
        scratch_shapes=[
            pltpu.VMEM(deep, f32),
            pltpu.VMEM(deep, f32),
            pltpu.VMEM((patches, members_here, cells), bf16),
        ],
        name="forecast",
    )(inside, prior, above, below, obs_index[0])

    observed = lax.all_to_all(observed, "mem", 0, 0, tiled=True).reshape(members, nobs)
    state = lax.all_to_all(state.astype(jnp.float16), "mem", 0, 0, tiled=True)
    own_index = lax.dynamic_index_in_dim(obs_index[0], lax.axis_index("mem"), 0, keepdims=True)
    high, low = pl.pallas_call(
        weights_kernel,
        out_shape=(shaped((members, members), bf16), shaped((members, members), bf16)),
        cost_estimate=pl.CostEstimate(flops=2 * 19 * members**3, bytes_accessed=2 * 1024 * 1024, transcendentals=0),
        name="weights",
    )(observed, own_index, obs_values[0], obs_var[0])
    analysed = pl.pallas_call(
        update_kernel, out_shape=shaped((members, cells), f32), name="update"
    )(state.astype(f32).reshape(members, cells), high, low)
    returned = lax.all_to_all(
        analysed.astype(jnp.float16).reshape(patches, members_here, cells), "mem", 0, 0, tiled=True
    )
    per_group = GROUP * fields * rows * cols // LANES
    out = pl.pallas_call(
        unpack_kernel,
        grid=(members_here // GROUP,),
        in_specs=[pl.BlockSpec((patches, GROUP, cells), lambda g: (0, g, 0))],
        out_specs=pl.BlockSpec((per_group, LANES), lambda g: (g, 0)),
        out_shape=shaped((members_here * fields * rows * cols // LANES, LANES), f32),
        name="unpack",
    )(returned.astype(f32))
    return untiled_view(out, prior_collection.shape)


def solution(mesh):
    in_specs = (
        P("mem", None, "band", None),
        P("band", None, None),
        P("band", "mem", None),
        P("band", "mem", None),
    )
    out_specs = P("mem", None, "band", None)
    return jax.shard_map(body, mesh=mesh, in_specs=in_specs, out_specs=out_specs, check_vma=False)
```

```python
import math

import jax
import jax.numpy as jnp
from jax import lax
from jax.experimental import pallas as pl
from jax.experimental.pallas import tpu as pltpu
from jax.sharding import PartitionSpec as P

STEPS = 3
NEWTON = 3
HALO = 2 * STEPS

time_step = 0.1
gravity = 1.0
coriolis = 0.05
mean_depth = 1.0

GROUP = 8
LANES = 128
BLOCK = 16
PASSES = 1


def tiled_view(x):
    m, f, r, c = x.shape
    halves = c // LANES
    return x.reshape(m, f, r, halves, LANES).transpose(0, 1, 3, 2, 4).reshape(-1, LANES)


def untiled_view(x, shape):
    m, f, r, c = shape
    halves = c // LANES
    return x.reshape(m, f, halves, r, LANES).transpose(0, 1, 3, 2, 4).reshape(shape)


def block_transpose(tiles):
    tiles = list(tiles)
    block = lax.broadcasted_iota(jnp.int32, tiles[0].shape, 1) // BLOCK
    for s in (4, 2, 1):
        high = (block & s) != 0
        for i in range(8):
            if i & s:
                continue
            a, b = tiles[i], tiles[i + s]
            tiles[i] = jnp.where(high, pltpu.roll(b, BLOCK * s, 1), a)
            tiles[i + s] = jnp.where(high, b, pltpu.roll(a, LANES - BLOCK * s, 1))
    return tiles


def edges_kernel(prior_ref, first_ref, last_ref):
    fields, rows = 3, 8
    stride = fields * rows * 2
    for member in range(0, first_ref.shape[1], 2 * GROUP):
        for f in range(fields):
            for half in range(2):
                lanes = slice(half * LANES, (half + 1) * LANES)
                for row in range(rows):
                    parts = [
                        prior_ref[pl.ds((m * fields + f) * 2 * rows + half * rows + row, GROUP, stride=stride), :]
                        for m in (member, member + GROUP)
                    ]
                    both = jnp.concatenate(parts, axis=0).astype(jnp.bfloat16)
                    if row < HALO:
                        first_ref[f * HALO + row, member : member + 2 * GROUP, lanes] = both
                    if row >= rows - HALO:
                        last_ref[f * HALO + row - (rows - HALO), member : member + 2 * GROUP, lanes] = both


def east_west(x):
    cols = x.shape[-1]
    return pltpu.roll(x, cols - 1, 1) - pltpu.roll(x, 1, 1)


def forecast_kernel(inside_ref, prior_ref, above_ref, below_ref, index_ref, exact_ref, sent_ref, ping, pong):
    fields, rows = 3, 8
    deep = rows + 2 * HALO
    stride = fields * rows * 2
    patches = sent_ref.shape[0]
    cells = fields * LANES
    above_in = inside_ref[0]
    below_in = inside_ref[1]
    half_step = 0.5 * time_step

    for f in range(fields):
        for row in range(HALO):
            ping[f * deep + row] = above_ref[f * HALO + row].astype(jnp.float32)
            ping[f * deep + HALO + rows + row] = below_ref[f * HALO + row].astype(jnp.float32)
        for half in range(2):
            for row in range(rows):
                start = f * 2 * rows + half * rows + row
                ping[f * deep + HALO + row, :, half * LANES : (half + 1) * LANES] = prior_ref[
                    pl.ds(start, GROUP, stride=stride), :
                ]

    def masked(x, row):
        if row < HALO:
            return x * above_in
        if row >= HALO + rows:
            return x * below_in
        return x

    src, dst = ping, pong
    for turn in range(STEPS):
        low = 2 * (turn + 1)
        high = deep - 2 * (turn + 1)
        north_flux = {}

        def flux(row):
            if row not in north_flux:
                north_flux[row] = (mean_depth + src[row]) * src[2 * deep + row]
            return north_flux[row]

        def new_height(row):
            height = src[row]
            flux_east = (mean_depth + height) * src[deep + row]
            return masked(height - half_step * (east_west(flux_east) + (flux(row + 1) - flux(row - 1))), row)

        heights = {row: new_height(row) for row in (low - 1, low)}
        for row in range(low, high):
            heights[row + 1] = new_height(row + 1)
            east = src[deep + row]
            north = src[2 * deep + row]
            east_slope = src[deep + row + 1] - src[deep + row - 1]
            north_slope = src[2 * deep + row + 1] - src[2 * deep + row - 1]
            height_slope = heights[row + 1] - heights[row - 1]
            new_east = (
                east
                - half_step * (gravity * east_west(heights[row]) + east * east_west(east) + north * east_slope)
                + coriolis * north
            )
            new_north = (
                north
                - half_step * (gravity * height_slope + east * east_west(north) + north * north_slope)
                - coriolis * east
            )
            dst[row] = heights[row]
            dst[deep + row] = masked(new_east, row)
            dst[2 * deep + row] = masked(new_north, row)
            del heights[row - 1]
        src, dst = dst, src

    for f in range(fields):
        for half in range(2):
            lanes = slice(half * LANES, (half + 1) * LANES)
            tiles = [src[f * deep + HALO + row, :, lanes] for row in range(rows)]
            for p, tile in enumerate(block_transpose(tiles)):
                exact_ref[half * 8 + p, :, f * LANES : (f + 1) * LANES] = tile
    for p in range(patches):
        sent_ref[p, :, :cells] = exact_ref[p].astype(jnp.bfloat16)

    index = index_ref[...]
    field_row = (index * 1366) >> 16
    column = index - field_row * (3 * BLOCK)
    tile_of = (column >> 4) * fields + (field_row >> 3)
    lane_of = (field_row & 7) * BLOCK + (column & (BLOCK - 1))
    for p in range(patches):
        for half in range(index.shape[1] // LANES):
            lanes = slice(half * LANES, (half + 1) * LANES)
            tile = jnp.broadcast_to(tile_of[p : p + 1, lanes], (GROUP, LANES))
            lane = jnp.broadcast_to(lane_of[p : p + 1, lanes], (GROUP, LANES))
            picked = None
            for k in range(3):
                for f in range(fields):
                    values = exact_ref[(p + k - 1) % patches, :, f * LANES : (f + 1) * LANES]
                    values = jnp.take_along_axis(values, lane, axis=1, mode="promise_in_bounds")
                    picked = values if picked is None else jnp.where(tile == k * fields + f, values, picked)
            sent_ref[p, :, cells + half * LANES : cells + (half + 1) * LANES] = picked.astype(jnp.bfloat16)


def split(x):
    high = x.astype(jnp.bfloat16)
    return high, (x - high.astype(jnp.float32)).astype(jnp.bfloat16)


def mul3(a, b):
    def dot(x, y):
        return jnp.dot(x, y, preferred_element_type=jnp.float32)

    return dot(a[0], b[0]) + (dot(a[0], b[1]) + dot(a[1], b[0]))


def three_rows(x):
    high = x.astype(jnp.bfloat16).astype(jnp.float32)
    rest = x - high
    middle = rest.astype(jnp.bfloat16).astype(jnp.float32)
    low = rest - middle
    shape = (16, x.shape[1])
    row = lax.broadcasted_iota(jnp.int32, shape, 0)
    stacked = jnp.where(row == 0, high, jnp.where(row == 1, middle, jnp.where(row == 2, low, 0.0)))
    return stacked.astype(jnp.bfloat16)


def analyse_kernel(here_ref, got_ref, index_ref, values_ref, var_ref, out_ref):
    members = got_ref.shape[0]
    cells = got_ref.shape[1] - values_ref.shape[1]
    wide = got_ref[:, cells:].astype(jnp.float32)
    obs_mean = jnp.sum(wide, axis=0, keepdims=True) * (1.0 / members)
    perturb = (wide - obs_mean).astype(jnp.bfloat16)
    index = index_ref[pl.ds(here_ref[0], 1), :]
    column = (index - ((index * 1366) >> 16) * (3 * BLOCK)).astype(jnp.float32)
    taper = jnp.exp(-0.5 * jnp.square((column - (3 * BLOCK - 1) * 0.5) / BLOCK))
    obs_weight = taper / var_ref[...]
    weighted = (perturb.astype(jnp.float32) * obs_weight).astype(jnp.bfloat16)
    contract = (((1,), (1,)), ((), ()))
    gram = lax.dot_general(perturb, weighted, contract, preferred_element_type=jnp.float32)
    row = lax.broadcasted_iota(jnp.int32, (members, members), 0)
    col = lax.broadcasted_iota(jnp.int32, (members, members), 1)
    on_diagonal = row == col
    lengths = jnp.sum(jnp.abs(gram), axis=0, keepdims=True)
    diagonal = jnp.sum(jnp.where(on_diagonal, gram, 0.0), axis=0, keepdims=True)
    lengths = lengths + (jnp.abs(diagonal + (members - 1)) - jnp.abs(diagonal))
    norm_bound = jnp.max(lengths, axis=1, keepdims=True)

    def mul(a, b):
        if PASSES == 3:
            rest = mul3(split(a[1]), split(b[1]))
        else:
            rest = jnp.dot(
                a[1].astype(jnp.bfloat16), b[1].astype(jnp.bfloat16), preferred_element_type=jnp.float32
            )
        return a[0] * b[0], a[0] * b[1] + b[0] * a[1] + rest

    def middle_of(a):
        return 1.5 - 0.5 * a[0], -0.5 * a[1]

    inverse_bound = 1.0 / norm_bound
    iterate = ((members - 1) * inverse_bound, gram * inverse_bound)
    middle = middle_of(iterate)
    inverse = middle
    for turn in range(1, NEWTON):
        iterate = mul(iterate, middle)
        middle = middle_of(mul(inverse, iterate))
        inverse = mul(middle, inverse)
    scale, rest = inverse
    rest_parts = split(rest)

    def through(x):
        rows = three_rows(x)
        both = jnp.dot(rows, rest_parts[0], preferred_element_type=jnp.float32) + jnp.dot(
            rows, rest_parts[1], preferred_element_type=jnp.float32
        )
        return scale * x + jnp.sum(both, axis=0, keepdims=True)

    innovation = obs_weight * (values_ref[...] - obs_mean)
    pulled = jnp.sum(
        lax.dot_general(three_rows(innovation), perturb, contract, preferred_element_type=jnp.float32),
        axis=0,
        keepdims=True,
    )
    mean_weight = through(through(pulled)) * inverse_bound
    grow = math.sqrt(members - 1) * lax.rsqrt(norm_bound)
    diagonal = jnp.sum(jnp.where(on_diagonal, rest, 0.0), axis=0, keepdims=True)
    average = jnp.sum(diagonal, axis=1, keepdims=True) * (1.0 / members)
    kept = (grow * (scale + average)).astype(jnp.bfloat16).astype(jnp.float32)
    change = grow * rest + mean_weight + jnp.where(on_diagonal, grow * scale - kept, 0.0)
    change = change.astype(jnp.bfloat16)

    fields = cells // LANES
    patches, here = out_ref.shape[0], members // out_ref.shape[0]
    state = got_ref[:, :cells].astype(jnp.float32)
    state_mean = jnp.sum(state, axis=0, keepdims=True) * (1.0 / members)
    high, low = split(state - state_mean)
    moved = (1.0 - kept) * state_mean + (
        jnp.dot(change, high, preferred_element_type=jnp.float32)
        + jnp.dot(change, low, preferred_element_type=jnp.float32)
    )
    kept_rows = jnp.broadcast_to(kept, (8, LANES)).astype(jnp.bfloat16)
    for p in range(patches):
        for f in range(fields):
            out_ref[p, f * here : (f + 1) * here, :] = moved[
                p * here : (p + 1) * here, f * LANES : (f + 1) * LANES
            ].astype(jnp.bfloat16)
        out_ref[p, fields * here :, :] = kept_rows


def unpack_kernel(returned_ref, exact_ref, out_ref):
    fields, rows = 3, 8
    stride = fields * rows * 2
    per_group = stride * GROUP
    here = (returned_ref.shape[1] - 8) // fields
    count = exact_ref.shape[1]
    first = pl.multiple_of(pl.program_id(0) * count, count)
    for f in range(fields):
        for half in range(2):
            tiles = []
            for p in range(half * 8, half * 8 + 8):
                moved = returned_ref[p, pl.ds(f * here + first, count), :].astype(jnp.float32)
                kept = returned_ref[p, fields * here : fields * here + 8, :].astype(jnp.float32)[0:1, :]
                tiles.append(moved + kept * exact_ref[p, :, f * LANES : (f + 1) * LANES])
            for r, tile in enumerate(block_transpose(tiles)):
                for g in range(count // GROUP):
                    start = g * per_group + f * 2 * rows + half * rows + r
                    out_ref[pl.ds(start, GROUP, stride=stride), :] = tile[g * GROUP : (g + 1) * GROUP]


def body(prior_collection, obs_index, obs_values, obs_var):
    members_here, fields, rows, cols = prior_collection.shape
    bands = lax.axis_size("band")
    patches = lax.axis_size("mem")
    members = members_here * patches
    nobs = obs_index.shape[-1]
    cells = fields * rows * BLOCK
    f32, bf16 = jnp.float32, jnp.bfloat16
    shaped = jax.ShapeDtypeStruct
    prior = tiled_view(prior_collection)

    halo_shape = (fields * HALO, members_here, cols)
    first, last = pl.pallas_call(
        edges_kernel, out_shape=(shaped(halo_shape, bf16), shaped(halo_shape, bf16)), name="edges"
    )(prior)
    up = [(i, i + 1) for i in range(bands - 1)]
    down = [(j, i) for i, j in up]
    above = lax.ppermute(last, "band", up)
    below = lax.ppermute(first, "band", down)

    band = lax.axis_index("band")
    inside = jnp.stack([band > 0, band < bands - 1]).astype(f32)
    vmem = pl.BlockSpec(memory_space=pltpu.VMEM)
    smem = pl.BlockSpec(memory_space=pltpu.SMEM)
    deep = (fields * (rows + 2 * HALO), GROUP, cols)
    groups = members_here // GROUP
    per_group = GROUP * fields * rows * cols // LANES

    def of_group(*shape):
        return pl.BlockSpec(shape, lambda g: (0, g, 0))

    exact, sent = pl.pallas_call(
        forecast_kernel,
        grid=(groups,),
        in_specs=[
            smem,
            pl.BlockSpec((per_group, LANES), lambda g: (g, 0)),
            of_group(fields * HALO, GROUP, cols),
            of_group(fields * HALO, GROUP, cols),
            pl.BlockSpec((patches, nobs), lambda g: (0, 0)),
        ],
        out_specs=[of_group(patches, GROUP, cells), of_group(patches, GROUP, cells + nobs)],
        out_shape=(
            shaped((patches, members_here, cells), f32),
            shaped((patches, members_here, cells + nobs), bf16),
        ),
        scratch_shapes=[pltpu.VMEM(deep, f32), pltpu.VMEM(deep, f32)],
        name="forecast",
    )(inside, prior, above, below, obs_index[0])

    got = lax.all_to_all(sent, "mem", 0, 0, tiled=True).reshape(members, cells + nobs)
    here = lax.axis_index("mem").astype(jnp.int32).reshape(1)
    moved = pl.pallas_call(
        analyse_kernel,
        in_specs=[smem, vmem, vmem, vmem, vmem],
        out_shape=shaped((patches, fields * members_here + 8, LANES), bf16),
        name="analyse",
    )(here, got, obs_index[0], obs_values[0], obs_var[0])
    returned = lax.all_to_all(moved, "mem", 0, 0, tiled=True)
    count = 2 * GROUP
    out = pl.pallas_call(
        unpack_kernel,
        grid=(members_here // count,),
        in_specs=[
            pl.BlockSpec((patches, fields * members_here + 8, LANES), lambda g: (0, 0, 0)),
            pl.BlockSpec((patches, count, cells), lambda g: (0, g, 0)),
        ],
        out_specs=pl.BlockSpec((2 * per_group, LANES), lambda g: (g, 0)),
        out_shape=shaped((members_here * fields * rows * cols // LANES, LANES), f32),
        name="unpack",
    )(returned, exact)
    return untiled_view(out, prior_collection.shape)


def solution(mesh):
    in_specs = (
        P("mem", None, "band", None),
        P("band", None, None),
        P("band", "mem", None),
        P("band", "mem", None),
    )
    out_specs = P("mem", None, "band", None)
    return jax.shard_map(body, mesh=mesh, in_specs=in_specs, out_specs=out_specs, check_vma=False)
```

```python
import math

import jax
import jax.numpy as jnp
from jax import lax
from jax.experimental import pallas as pl
from jax.experimental.pallas import tpu as pltpu
from jax.sharding import PartitionSpec as P

STEPS = 3
NEWTON = 3
HALO = 2 * STEPS

time_step = 0.1
gravity = 1.0
coriolis = 0.05
mean_depth = 1.0

GROUP = 8
LANES = 128
BLOCK = 16
PASSES = 1


def in_vmem(shape, dtype):
    return pltpu.VMEM(shape, dtype)


def to_vmem(x):
    return pltpu.with_memory_space_constraint(x, pltpu.VMEM)


def tiled_view(x):
    m, f, r, c = x.shape
    halves = c // LANES
    return x.reshape(m, f, r, halves, LANES).transpose(0, 1, 3, 2, 4).reshape(-1, LANES)


def untiled_view(x, shape):
    m, f, r, c = shape
    halves = c // LANES
    return x.reshape(m, f, halves, r, LANES).transpose(0, 1, 3, 2, 4).reshape(shape)


def block_transpose(tiles):
    tiles = list(tiles)
    block = lax.broadcasted_iota(jnp.int32, tiles[0].shape, 1) // BLOCK
    for s in (4, 2, 1):
        high = (block & s) != 0
        for i in range(8):
            if i & s:
                continue
            a, b = tiles[i], tiles[i + s]
            tiles[i] = jnp.where(high, pltpu.roll(b, BLOCK * s, 1), a)
            tiles[i + s] = jnp.where(high, b, pltpu.roll(a, LANES - BLOCK * s, 1))
    return tiles


def edges_kernel(prior_ref, first_ref, last_ref):
    fields, rows = 3, 8
    stride = fields * rows * 2
    for member in range(0, first_ref.shape[1], 2 * GROUP):
        for f in range(fields):
            for half in range(2):
                lanes = slice(half * LANES, (half + 1) * LANES)
                for row in range(rows):
                    parts = [
                        prior_ref[pl.ds((m * fields + f) * 2 * rows + half * rows + row, GROUP, stride=stride), :]
                        for m in (member, member + GROUP)
                    ]
                    both = jnp.concatenate(parts, axis=0).astype(jnp.bfloat16)
                    if row < HALO:
                        first_ref[f * HALO + row, member : member + 2 * GROUP, lanes] = both
                    if row >= rows - HALO:
                        last_ref[f * HALO + row - (rows - HALO), member : member + 2 * GROUP, lanes] = both


def window_spots(index):
    field_row = (index * 1366) >> 16
    column = index - field_row * (3 * BLOCK)
    return (column >> 4) * (3 * LANES) + field_row * BLOCK + (column & (BLOCK - 1))


def stage_kernel(prior_ref, index_ref, own_ref, chosen_ref):
    fields, rows = 3, 8
    stride = fields * rows * 2
    for member in range(0, own_ref.shape[1], GROUP):
        for f in range(fields):
            for half in range(2):
                for row in range(rows):
                    start = (member * fields + f) * 2 * rows + half * rows + row
                    own_ref[f * rows + row, member : member + GROUP, half * LANES : (half + 1) * LANES] = prior_ref[
                        pl.ds(start, GROUP, stride=stride), :
                    ]
    spots = window_spots(index_ref[...])
    order = lax.broadcasted_iota(jnp.int32, chosen_ref.shape[1:], 0)
    for p in range(chosen_ref.shape[0]):
        chosen_ref[p] = jnp.where(order == spots[p : p + 1, :], 1.0, 0.0).astype(jnp.bfloat16)


def east_west(x):
    cols = x.shape[-1]
    return pltpu.roll(x, cols - 1, 1) - pltpu.roll(x, 1, 1)


def forecast_kernel(inside_ref, own_ref, above_ref, below_ref, chosen_ref, exact_ref, sent_ref, ping, pong):
    fields, rows = 3, 8
    deep = rows + 2 * HALO
    patches = sent_ref.shape[0]
    cells = fields * LANES
    above_in = inside_ref[0]
    below_in = inside_ref[1]
    half_step = 0.5 * time_step
    here = pl.ds(pl.multiple_of(pl.program_id(0) * GROUP, GROUP), GROUP)

    for f in range(fields):
        for row in range(HALO):
            ping[f * deep + row] = above_ref[f * HALO + row, here, :].astype(jnp.float32)
            ping[f * deep + HALO + rows + row] = below_ref[f * HALO + row, here, :].astype(jnp.float32)
        for row in range(rows):
            ping[f * deep + HALO + row] = own_ref[f * rows + row, here, :]

    def masked(x, row):
        if row < HALO:
            return x * above_in
        if row >= HALO + rows:
            return x * below_in
        return x

    src, dst = ping, pong
    for turn in range(STEPS):
        low = 2 * (turn + 1)
        high = deep - 2 * (turn + 1)
        north_flux = {}

        def flux(row):
            if row not in north_flux:
                north_flux[row] = (mean_depth + src[row]) * src[2 * deep + row]
            return north_flux[row]

        def new_height(row):
            height = src[row]
            flux_east = (mean_depth + height) * src[deep + row]
            return masked(height - half_step * (east_west(flux_east) + (flux(row + 1) - flux(row - 1))), row)

        heights = {row: new_height(row) for row in (low - 1, low)}
        for row in range(low, high):
            heights[row + 1] = new_height(row + 1)
            east = src[deep + row]
            north = src[2 * deep + row]
            east_slope = src[deep + row + 1] - src[deep + row - 1]
            north_slope = src[2 * deep + row + 1] - src[2 * deep + row - 1]
            height_slope = heights[row + 1] - heights[row - 1]
            new_east = (
                east
                - half_step * (gravity * east_west(heights[row]) + east * east_west(east) + north * east_slope)
                + coriolis * north
            )
            new_north = (
                north
                - half_step * (gravity * height_slope + east * east_west(north) + north * north_slope)
                - coriolis * east
            )
            dst[row] = heights[row]
            dst[deep + row] = masked(new_east, row)
            dst[2 * deep + row] = masked(new_north, row)
            del heights[row - 1]
        src, dst = dst, src

    for f in range(fields):
        for half in range(2):
            lanes = slice(half * LANES, (half + 1) * LANES)
            tiles = [src[f * deep + HALO + row, :, lanes] for row in range(rows)]
            for p, tile in enumerate(block_transpose(tiles)):
                exact_ref[half * 8 + p, here, f * LANES : (f + 1) * LANES] = tile
    for p in range(patches):
        sent_ref[p, here, :cells] = exact_ref[p, here, :].astype(jnp.bfloat16)

    @pl.when(pl.program_id(0) == pl.num_programs(0) - 1)
    def _():
        for p in range(patches):
            total = None
            for k in range(3):
                piece = jnp.dot(
                    sent_ref[(p + k - 1) % patches, :, :cells],
                    chosen_ref[p, k * cells : (k + 1) * cells, :],
                    preferred_element_type=jnp.float32,
                )
                total = piece if total is None else total + piece
            sent_ref[p, :, cells:] = total.astype(jnp.bfloat16)


def split(x):
    high = x.astype(jnp.bfloat16)
    return high, (x - high.astype(jnp.float32)).astype(jnp.bfloat16)


def mul3(a, b):
    def dot(x, y):
        return jnp.dot(x, y, preferred_element_type=jnp.float32)

    return dot(a[0], b[0]) + (dot(a[0], b[1]) + dot(a[1], b[0]))


def three_rows(x):
    high = x.astype(jnp.bfloat16).astype(jnp.float32)
    rest = x - high
    middle = rest.astype(jnp.bfloat16).astype(jnp.float32)
    low = rest - middle
    shape = (16, x.shape[1])
    row = lax.broadcasted_iota(jnp.int32, shape, 0)
    stacked = jnp.where(row == 0, high, jnp.where(row == 1, middle, jnp.where(row == 2, low, 0.0)))
    return stacked.astype(jnp.bfloat16)


def analyse_kernel(here_ref, got_ref, index_ref, values_ref, var_ref, out_ref):
    members = got_ref.shape[0]
    cells = got_ref.shape[1] - values_ref.shape[1]
    wide = got_ref[:, cells:].astype(jnp.float32)
    obs_mean = jnp.sum(wide, axis=0, keepdims=True) * (1.0 / members)
    perturb = (wide - obs_mean).astype(jnp.bfloat16)
    index = index_ref[pl.ds(here_ref[0], 1), :]
    column = (index - ((index * 1366) >> 16) * (3 * BLOCK)).astype(jnp.float32)
    taper = jnp.exp(-0.5 * jnp.square((column - (3 * BLOCK - 1) * 0.5) / BLOCK))
    obs_weight = taper / var_ref[...]
    weighted = (perturb.astype(jnp.float32) * obs_weight).astype(jnp.bfloat16)
    contract = (((1,), (1,)), ((), ()))
    gram = lax.dot_general(perturb, weighted, contract, preferred_element_type=jnp.float32)
    row = lax.broadcasted_iota(jnp.int32, (members, members), 0)
    col = lax.broadcasted_iota(jnp.int32, (members, members), 1)
    on_diagonal = row == col
    lengths = jnp.sum(jnp.abs(gram), axis=0, keepdims=True)
    diagonal = jnp.sum(jnp.where(on_diagonal, gram, 0.0), axis=0, keepdims=True)
    lengths = lengths + (jnp.abs(diagonal + (members - 1)) - jnp.abs(diagonal))
    norm_bound = jnp.max(lengths, axis=1, keepdims=True)

    def mul(a, b):
        if PASSES == 3:
            rest = mul3(split(a[1]), split(b[1]))
        else:
            rest = jnp.dot(
                a[1].astype(jnp.bfloat16), b[1].astype(jnp.bfloat16), preferred_element_type=jnp.float32
            )
        return a[0] * b[0], a[0] * b[1] + b[0] * a[1] + rest

    def middle_of(a):
        return 1.5 - 0.5 * a[0], -0.5 * a[1]

    inverse_bound = 1.0 / norm_bound
    iterate = ((members - 1) * inverse_bound, gram * inverse_bound)
    middle = middle_of(iterate)
    inverse = middle
    for turn in range(1, NEWTON):
        iterate = mul(iterate, middle)
        middle = middle_of(mul(inverse, iterate))
        inverse = mul(middle, inverse)
    scale, rest = inverse
    rest_parts = split(rest)

    def through(x):
        rows = three_rows(x)
        both = jnp.dot(rows, rest_parts[0], preferred_element_type=jnp.float32) + jnp.dot(
            rows, rest_parts[1], preferred_element_type=jnp.float32
        )
        return scale * x + jnp.sum(both, axis=0, keepdims=True)

    innovation = obs_weight * (values_ref[...] - obs_mean)
    pulled = jnp.sum(
        lax.dot_general(three_rows(innovation), perturb, contract, preferred_element_type=jnp.float32),
        axis=0,
        keepdims=True,
    )
    mean_weight = through(through(pulled)) * inverse_bound
    grow = math.sqrt(members - 1) * lax.rsqrt(norm_bound)
    diagonal = jnp.sum(jnp.where(on_diagonal, rest, 0.0), axis=0, keepdims=True)
    average = jnp.sum(diagonal, axis=1, keepdims=True) * (1.0 / members)
    kept = (grow * (scale + average)).astype(jnp.bfloat16).astype(jnp.float32)
    change = grow * rest + mean_weight + jnp.where(on_diagonal, grow * scale - kept, 0.0)
    change = change.astype(jnp.bfloat16)

    fields = cells // LANES
    patches, here = out_ref.shape[0], members // out_ref.shape[0]
    state = got_ref[:, :cells].astype(jnp.float32)
    state_mean = jnp.sum(state, axis=0, keepdims=True) * (1.0 / members)
    high, low = split(state - state_mean)
    moved = (1.0 - kept) * state_mean + (
        jnp.dot(change, high, preferred_element_type=jnp.float32)
        + jnp.dot(change, low, preferred_element_type=jnp.float32)
    )
    kept_rows = jnp.broadcast_to(kept, (8, LANES)).astype(jnp.bfloat16)
    for p in range(patches):
        for f in range(fields):
            out_ref[p, f * here : (f + 1) * here, :] = moved[
                p * here : (p + 1) * here, f * LANES : (f + 1) * LANES
            ].astype(jnp.bfloat16)
        out_ref[p, fields * here :, :] = kept_rows


def unpack_kernel(returned_ref, exact_ref, out_ref):
    fields, rows = 3, 8
    count = 2 * GROUP
    stride = fields * rows * 2
    per_group = stride * GROUP
    here = (returned_ref.shape[1] - 8) // fields
    first = pl.multiple_of(pl.program_id(0) * count, count)
    for f in range(fields):
        for half in range(2):
            tiles = []
            for p in range(half * 8, half * 8 + 8):
                moved = returned_ref[p, pl.ds(f * here + first, count), :].astype(jnp.float32)
                kept = returned_ref[p, fields * here : fields * here + 8, :].astype(jnp.float32)[0:1, :]
                tiles.append(moved + kept * exact_ref[p, pl.ds(first, count), f * LANES : (f + 1) * LANES])
            for r, tile in enumerate(block_transpose(tiles)):
                for g in range(count // GROUP):
                    start = g * per_group + f * 2 * rows + half * rows + r
                    out_ref[pl.ds(start, GROUP, stride=stride), :] = tile[g * GROUP : (g + 1) * GROUP]


def body(prior_collection, obs_index, obs_values, obs_var):
    members_here, fields, rows, cols = prior_collection.shape
    bands = lax.axis_size("band")
    patches = lax.axis_size("mem")
    members = members_here * patches
    nobs = obs_index.shape[-1]
    cells = fields * rows * BLOCK
    f32, bf16 = jnp.float32, jnp.bfloat16
    shaped = jax.ShapeDtypeStruct
    prior = tiled_view(prior_collection)

    halo_shape = (fields * HALO, members_here, cols)
    vmem = pl.BlockSpec(memory_space=pltpu.VMEM)
    smem = pl.BlockSpec(memory_space=pltpu.SMEM)
    first, last = pl.pallas_call(
        edges_kernel,
        out_specs=[vmem, vmem],
        out_shape=(in_vmem(halo_shape, bf16), in_vmem(halo_shape, bf16)),
        name="edges",
    )(prior)
    up = [(i, i + 1) for i in range(bands - 1)]
    down = [(j, i) for i, j in up]
    above = lax.ppermute(last, "band", up)
    below = lax.ppermute(first, "band", down)

    own, chosen = pl.pallas_call(
        stage_kernel,
        out_specs=[vmem, vmem],
        out_shape=(
            in_vmem((fields * rows, members_here, cols), f32),
            in_vmem((patches, 3 * cells, nobs), bf16),
        ),
        cost_estimate=pl.CostEstimate(flops=10**8, bytes_accessed=10**6, transcendentals=0),
        compiler_params=pltpu.CompilerParams(vmem_limit_bytes=24 * 1024 * 1024),
        name="stage",
    )(prior, obs_index[0])

    band = lax.axis_index("band")
    inside = jnp.stack([band > 0, band < bands - 1]).astype(f32)
    deep = (fields * (rows + 2 * HALO), GROUP, cols)
    groups = members_here // GROUP
    per_group = GROUP * fields * rows * cols // LANES

    exact, sent = pl.pallas_call(
        forecast_kernel,
        grid=(groups,),
        in_specs=[
            smem,
            vmem,
            vmem,
            vmem,
            vmem,
        ],
        out_specs=[vmem, vmem],
        out_shape=(
            in_vmem((patches, members_here, cells), f32),
            in_vmem((patches, members_here, cells + nobs), bf16),
        ),
        scratch_shapes=[pltpu.VMEM(deep, f32), pltpu.VMEM(deep, f32)],
        compiler_params=pltpu.CompilerParams(vmem_limit_bytes=24 * 1024 * 1024),
        name="forecast",
    )(inside, to_vmem(own), to_vmem(above), to_vmem(below), to_vmem(chosen))

    got = lax.all_to_all(sent, "mem", 0, 0, tiled=True).reshape(members, cells + nobs)
    here = lax.axis_index("mem").astype(jnp.int32).reshape(1)
    moved = pl.pallas_call(
        analyse_kernel,
        in_specs=[smem, vmem, vmem, vmem, vmem],
        out_specs=vmem,
        out_shape=in_vmem((patches, fields * members_here + 8, LANES), bf16),
        name="analyse",
    )(here, to_vmem(got), obs_index[0], obs_values[0], obs_var[0])
    returned = lax.all_to_all(moved, "mem", 0, 0, tiled=True)
    count = 2 * GROUP
    out = pl.pallas_call(
        unpack_kernel,
        grid=(members_here // count,),
        in_specs=[
            vmem,
            vmem,
        ],
        out_specs=pl.BlockSpec((2 * per_group, LANES), lambda g: (g, 0)),
        out_shape=shaped((members_here * fields * rows * cols // LANES, LANES), f32),
        name="unpack",
    )(to_vmem(returned), to_vmem(exact))
    return untiled_view(out, prior_collection.shape)


def solution(mesh):
    in_specs = (
        P("mem", None, "band", None),
        P("band", None, None),
        P("band", "mem", None),
        P("band", "mem", None),
    )
    out_specs = P("mem", None, "band", None)
    return jax.shard_map(body, mesh=mesh, in_specs=in_specs, out_specs=out_specs, check_vma=False)
```

```python
import math

import jax
import jax.numpy as jnp
from jax import lax
from jax.experimental import pallas as pl
from jax.experimental.pallas import tpu as pltpu
from jax.sharding import PartitionSpec as P

STEPS = 3
NEWTON = 3
HALO = 2 * STEPS

time_step = 0.1
gravity = 1.0
coriolis = 0.05
mean_depth = 1.0

GROUP = 8
LANES = 128
BLOCK = 16
PASSES = 1


def in_vmem(shape, dtype):
    return pltpu.VMEM(shape, dtype)


def to_vmem(x):
    return pltpu.with_memory_space_constraint(x, pltpu.VMEM)


def tiled_view(x):
    m, f, r, c = x.shape
    halves = c // LANES
    return x.reshape(m, f, r, halves, LANES).transpose(0, 1, 3, 2, 4).reshape(-1, LANES)


def untiled_view(x, shape):
    m, f, r, c = shape
    halves = c // LANES
    return x.reshape(m, f, halves, r, LANES).transpose(0, 1, 3, 2, 4).reshape(shape)


def block_transpose(tiles):
    tiles = list(tiles)
    block = lax.broadcasted_iota(jnp.int32, tiles[0].shape, 1) // BLOCK
    for s in (4, 2, 1):
        high = (block & s) != 0
        for i in range(8):
            if i & s:
                continue
            a, b = tiles[i], tiles[i + s]
            tiles[i] = jnp.where(high, pltpu.roll(b, BLOCK * s, 1), a)
            tiles[i + s] = jnp.where(high, b, pltpu.roll(a, LANES - BLOCK * s, 1))
    return tiles


def edges_kernel(prior_ref, first_ref, last_ref, own_ref):
    fields, rows = 3, 8
    stride = fields * rows * 2
    for member in range(0, first_ref.shape[1], 2 * GROUP):
        for f in range(fields):
            for half in range(2):
                lanes = slice(half * LANES, (half + 1) * LANES)
                for row in range(rows):
                    parts = [
                        prior_ref[pl.ds((m * fields + f) * 2 * rows + half * rows + row, GROUP, stride=stride), :]
                        for m in (member, member + GROUP)
                    ]
                    both = jnp.concatenate(parts, axis=0)
                    own_ref[f * rows + row, member : member + 2 * GROUP, lanes] = both
                    both = both.astype(jnp.bfloat16)
                    if row < HALO:
                        first_ref[f * HALO + row, member : member + 2 * GROUP, lanes] = both
                    if row >= rows - HALO:
                        last_ref[f * HALO + row - (rows - HALO), member : member + 2 * GROUP, lanes] = both


def window_spots(index):
    field_row = (index * 1366) >> 16
    column = index - field_row * (3 * BLOCK)
    return (column >> 4) * (3 * LANES) + field_row * BLOCK + (column & (BLOCK - 1))


def stage_kernel(index_ref, chosen_ref):
    spots = window_spots(index_ref[...])
    order = lax.broadcasted_iota(jnp.int32, chosen_ref.shape[1:], 0)
    for p in range(chosen_ref.shape[0]):
        chosen_ref[p] = jnp.where(order == spots[p : p + 1, :], 1.0, 0.0).astype(jnp.bfloat16)


def east_west(x):
    cols = x.shape[-1]
    return pltpu.roll(x, cols - 1, 1) - pltpu.roll(x, 1, 1)


def forecast_kernel(place_ref, own_ref, above_ref, below_ref, chosen_ref, exact_ref, sent_ref, ping, pong):
    fields, rows = 3, 8
    deep = rows + 2 * HALO
    patches = sent_ref.shape[0]
    cells = fields * LANES
    above_in = place_ref[0].astype(jnp.float32)
    below_in = place_ref[1].astype(jnp.float32)
    half_step = 0.5 * time_step
    here = pl.ds(pl.multiple_of(pl.program_id(0) * GROUP, GROUP), GROUP)

    for f in range(fields):
        for row in range(HALO):
            ping[f * deep + row] = above_ref[f * HALO + row, here, :].astype(jnp.float32)
            ping[f * deep + HALO + rows + row] = below_ref[f * HALO + row, here, :].astype(jnp.float32)
        for row in range(rows):
            ping[f * deep + HALO + row] = own_ref[f * rows + row, here, :]

    def masked(x, row):
        if row < HALO:
            return x * above_in
        if row >= HALO + rows:
            return x * below_in
        return x

    src, dst = ping, pong
    for turn in range(STEPS):
        low = 2 * (turn + 1)
        high = deep - 2 * (turn + 1)
        north_flux = {}

        def flux(row):
            if row not in north_flux:
                north_flux[row] = (mean_depth + src[row]) * src[2 * deep + row]
            return north_flux[row]

        def new_height(row):
            height = src[row]
            flux_east = (mean_depth + height) * src[deep + row]
            return masked(height - half_step * (east_west(flux_east) + (flux(row + 1) - flux(row - 1))), row)

        heights = {row: new_height(row) for row in (low - 1, low)}
        for row in range(low, high):
            heights[row + 1] = new_height(row + 1)
            east = src[deep + row]
            north = src[2 * deep + row]
            east_slope = src[deep + row + 1] - src[deep + row - 1]
            north_slope = src[2 * deep + row + 1] - src[2 * deep + row - 1]
            height_slope = heights[row + 1] - heights[row - 1]
            new_east = (
                east
                - half_step * (gravity * east_west(heights[row]) + east * east_west(east) + north * east_slope)
                + coriolis * north
            )
            new_north = (
                north
                - half_step * (gravity * height_slope + east * east_west(north) + north * north_slope)
                - coriolis * east
            )
            dst[row] = heights[row]
            dst[deep + row] = masked(new_east, row)
            dst[2 * deep + row] = masked(new_north, row)
            del heights[row - 1]
        src, dst = dst, src

    for f in range(fields):
        for half in range(2):
            lanes = slice(half * LANES, (half + 1) * LANES)
            tiles = [src[f * deep + HALO + row, :, lanes] for row in range(rows)]
            for p, tile in enumerate(block_transpose(tiles)):
                exact_ref[half * 8 + p, here, f * LANES : (f + 1) * LANES] = tile
    for p in range(patches):
        sent_ref[p, here, :cells] = exact_ref[p, here, :].astype(jnp.bfloat16)

    @pl.when(pl.program_id(0) == pl.num_programs(0) - 1)
    def _():
        for p in range(patches):
            total = None
            for k in range(3):
                piece = jnp.dot(
                    sent_ref[(p + k - 1) % patches, :, :cells],
                    chosen_ref[p, k * cells : (k + 1) * cells, :],
                    preferred_element_type=jnp.float32,
                )
                total = piece if total is None else total + piece
            sent_ref[p, :, cells:] = total.astype(jnp.bfloat16)


def split(x):
    high = x.astype(jnp.bfloat16)
    return high, (x - high.astype(jnp.float32)).astype(jnp.bfloat16)


def mul3(a, b):
    def dot(x, y):
        return jnp.dot(x, y, preferred_element_type=jnp.float32)

    return dot(a[0], b[0]) + (dot(a[0], b[1]) + dot(a[1], b[0]))


def three_rows(x):
    high = x.astype(jnp.bfloat16).astype(jnp.float32)
    rest = x - high
    middle = rest.astype(jnp.bfloat16).astype(jnp.float32)
    low = rest - middle
    shape = (16, x.shape[1])
    row = lax.broadcasted_iota(jnp.int32, shape, 0)
    stacked = jnp.where(row == 0, high, jnp.where(row == 1, middle, jnp.where(row == 2, low, 0.0)))
    return stacked.astype(jnp.bfloat16)


def analyse_kernel(place_ref, got_ref, index_ref, values_ref, var_ref, out_ref):
    members = got_ref.shape[0]
    cells = got_ref.shape[1] - values_ref.shape[1]
    wide = got_ref[:, cells:].astype(jnp.float32)
    obs_mean = jnp.sum(wide, axis=0, keepdims=True) * (1.0 / members)
    perturb = (wide - obs_mean).astype(jnp.bfloat16)
    index = index_ref[pl.ds(place_ref[2], 1), :]
    column = (index - ((index * 1366) >> 16) * (3 * BLOCK)).astype(jnp.float32)
    taper = jnp.exp(-0.5 * jnp.square((column - (3 * BLOCK - 1) * 0.5) / BLOCK))
    obs_weight = taper / var_ref[...]
    weighted = (perturb.astype(jnp.float32) * obs_weight).astype(jnp.bfloat16)
    contract = (((1,), (1,)), ((), ()))
    gram = lax.dot_general(perturb, weighted, contract, preferred_element_type=jnp.float32)
    row = lax.broadcasted_iota(jnp.int32, (members, members), 0)
    col = lax.broadcasted_iota(jnp.int32, (members, members), 1)
    on_diagonal = row == col
    lengths = jnp.sum(jnp.abs(gram), axis=0, keepdims=True)
    diagonal = jnp.sum(jnp.where(on_diagonal, gram, 0.0), axis=0, keepdims=True)
    lengths = lengths + (jnp.abs(diagonal + (members - 1)) - jnp.abs(diagonal))
    norm_bound = jnp.max(lengths, axis=1, keepdims=True)

    def mul(a, b):
        if PASSES == 3:
            rest = mul3(split(a[1]), split(b[1]))
        else:
            rest = jnp.dot(
                a[1].astype(jnp.bfloat16), b[1].astype(jnp.bfloat16), preferred_element_type=jnp.float32
            )
        return a[0] * b[0], a[0] * b[1] + b[0] * a[1] + rest

    def middle_of(a):
        return 1.5 - 0.5 * a[0], -0.5 * a[1]

    inverse_bound = 1.0 / norm_bound
    iterate = ((members - 1) * inverse_bound, gram * inverse_bound)
    middle = middle_of(iterate)
    inverse = middle
    for turn in range(1, NEWTON):
        iterate = mul(iterate, middle)
        middle = middle_of(mul(inverse, iterate))
        inverse = mul(middle, inverse)
    scale, rest = inverse
    rest_parts = split(rest)

    def through(x):
        rows = three_rows(x)
        both = jnp.dot(rows, rest_parts[0], preferred_element_type=jnp.float32) + jnp.dot(
            rows, rest_parts[1], preferred_element_type=jnp.float32
        )
        return scale * x + jnp.sum(both, axis=0, keepdims=True)

    innovation = obs_weight * (values_ref[...] - obs_mean)
    pulled = jnp.sum(
        lax.dot_general(three_rows(innovation), perturb, contract, preferred_element_type=jnp.float32),
        axis=0,
        keepdims=True,
    )
    mean_weight = through(through(pulled)) * inverse_bound
    grow = math.sqrt(members - 1) * lax.rsqrt(norm_bound)
    diagonal = jnp.sum(jnp.where(on_diagonal, rest, 0.0), axis=0, keepdims=True)
    average = jnp.sum(diagonal, axis=1, keepdims=True) * (1.0 / members)
    kept = (grow * (scale + average)).astype(jnp.bfloat16).astype(jnp.float32)
    change = grow * rest + mean_weight + jnp.where(on_diagonal, grow * scale - kept, 0.0)
    change = change.astype(jnp.bfloat16)

    fields = cells // LANES
    patches, here = out_ref.shape[0], members // out_ref.shape[0]
    state = got_ref[:, :cells].astype(jnp.float32)
    state_mean = jnp.sum(state, axis=0, keepdims=True) * (1.0 / members)
    high, low = split(state - state_mean)
    moved = (1.0 - kept) * state_mean + (
        jnp.dot(change, high, preferred_element_type=jnp.float32)
        + jnp.dot(change, low, preferred_element_type=jnp.float32)
    )
    kept_rows = jnp.broadcast_to(kept, (8, LANES)).astype(jnp.bfloat16)
    for p in range(patches):
        for f in range(fields):
            out_ref[p, f * here : (f + 1) * here, :] = moved[
                p * here : (p + 1) * here, f * LANES : (f + 1) * LANES
            ].astype(jnp.bfloat16)
        out_ref[p, fields * here :, :] = kept_rows


def unpack_kernel(returned_ref, exact_ref, out_ref):
    fields, rows = 3, 8
    count = 2 * GROUP
    stride = fields * rows * 2
    per_group = stride * GROUP
    here = (returned_ref.shape[1] - 8) // fields
    first = pl.multiple_of(pl.program_id(0) * count, count)
    for f in range(fields):
        for half in range(2):
            tiles = []
            for p in range(half * 8, half * 8 + 8):
                moved = returned_ref[p, pl.ds(f * here + first, count), :].astype(jnp.float32)
                kept = returned_ref[p, fields * here : fields * here + 8, :].astype(jnp.float32)[0:1, :]
                tiles.append(moved + kept * exact_ref[p, pl.ds(first, count), f * LANES : (f + 1) * LANES])
            for r, tile in enumerate(block_transpose(tiles)):
                for g in range(count // GROUP):
                    start = g * per_group + f * 2 * rows + half * rows + r
                    out_ref[pl.ds(start, GROUP, stride=stride), :] = tile[g * GROUP : (g + 1) * GROUP]


def body(prior_collection, obs_index, obs_values, obs_var):
    members_here, fields, rows, cols = prior_collection.shape
    bands = lax.axis_size("band")
    patches = lax.axis_size("mem")
    members = members_here * patches
    nobs = obs_index.shape[-1]
    cells = fields * rows * BLOCK
    f32, bf16 = jnp.float32, jnp.bfloat16
    shaped = jax.ShapeDtypeStruct
    prior = tiled_view(prior_collection)

    halo_shape = (fields * HALO, members_here, cols)
    vmem = pl.BlockSpec(memory_space=pltpu.VMEM)
    smem = pl.BlockSpec(memory_space=pltpu.SMEM)
    first, last, own = pl.pallas_call(
        edges_kernel,
        out_specs=[vmem, vmem, vmem],
        out_shape=(
            in_vmem(halo_shape, bf16),
            in_vmem(halo_shape, bf16),
            in_vmem((fields * rows, members_here, cols), f32),
        ),
        name="edges",
    )(prior)
    up = [(i, i + 1) for i in range(bands - 1)]
    down = [(j, i) for i, j in up]
    above = lax.ppermute(last, "band", up)
    below = lax.ppermute(first, "band", down)

    chosen = pl.pallas_call(
        stage_kernel,
        out_specs=vmem,
        out_shape=in_vmem((patches, 3 * cells, nobs), bf16),
        cost_estimate=pl.CostEstimate(flops=10**8, bytes_accessed=10**6, transcendentals=0),
        compiler_params=pltpu.CompilerParams(vmem_limit_bytes=24 * 1024 * 1024),
        name="stage",
    )(obs_index[0])

    band = lax.axis_index("band")
    place = jnp.stack([band > 0, band < bands - 1, lax.axis_index("mem")]).astype(jnp.int32)
    deep = (fields * (rows + 2 * HALO), GROUP, cols)
    groups = members_here // GROUP
    per_group = GROUP * fields * rows * cols // LANES

    exact, sent = pl.pallas_call(
        forecast_kernel,
        grid=(groups,),
        in_specs=[
            smem,
            vmem,
            vmem,
            vmem,
            vmem,
        ],
        out_specs=[vmem, vmem],
        out_shape=(
            in_vmem((patches, members_here, cells), f32),
            in_vmem((patches, members_here, cells + nobs), bf16),
        ),
        scratch_shapes=[pltpu.VMEM(deep, f32), pltpu.VMEM(deep, f32)],
        compiler_params=pltpu.CompilerParams(vmem_limit_bytes=24 * 1024 * 1024),
        name="forecast",
    )(place, to_vmem(own), to_vmem(above), to_vmem(below), to_vmem(chosen))

    got = lax.all_to_all(sent, "mem", 0, 0, tiled=True).reshape(members, cells + nobs)
    moved = pl.pallas_call(
        analyse_kernel,
        in_specs=[smem, vmem, vmem, vmem, vmem],
        out_specs=vmem,
        out_shape=in_vmem((patches, fields * members_here + 8, LANES), bf16),
        name="analyse",
    )(place, to_vmem(got), obs_index[0], obs_values[0], obs_var[0])
    returned = lax.all_to_all(moved, "mem", 0, 0, tiled=True)
    count = 2 * GROUP
    out = pl.pallas_call(
        unpack_kernel,
        grid=(members_here // count,),
        in_specs=[
            vmem,
            vmem,
        ],
        out_specs=pl.BlockSpec((2 * per_group, LANES), lambda g: (g, 0)),
        out_shape=shaped((members_here * fields * rows * cols // LANES, LANES), f32),
        name="unpack",
    )(to_vmem(returned), to_vmem(exact))
    return untiled_view(out, prior_collection.shape)


def solution(mesh):
    in_specs = (
        P("mem", None, "band", None),
        P("band", None, None),
        P("band", "mem", None),
        P("band", "mem", None),
    )
    out_specs = P("mem", None, "band", None)
    return jax.shard_map(body, mesh=mesh, in_specs=in_specs, out_specs=out_specs, check_vma=False)
```
